32 devices in a mesh: dp: 1 (over z), wg: 32 (over y, x, core).
Axes of the slice: x: 4, y: 4, z: 1, core: 2. Of those that a mesh axis runs over, the one named last changes fastest.
The devices are a block of a 4x4x8 slice.
Arguments:
- hidden: bfloat16 [65536, 1024], P(('dp', 'wg'))
- choice: int32 [65536, 8], P(('dp', 'wg'))
- pre_scale: float32 [1024], replicated
- w_router: bfloat16 [1024, 32], replicated
- w_gelu: bfloat16 [32, 1024, 512], P(None, None, 'wg')
- w_linear: bfloat16 [32, 1024, 512], P(None, None, 'wg')
- w_down: bfloat16 [32, 512, 1024], P(None, 'wg')
- post_scale: float32 [1024], replicated
Outputs:
- output: bfloat16 [65536, 1024], P(('dp', 'wg'))
All inputs are finite; a program needn't handle non-finite values.
Results may differ from the reference program's by a relative error of at most 0.001.
Values are sent between devices in bfloat16 or wider.
A program may use at most 768 MiB of HBM per device.

```python
import jax
import jax.numpy as jnp
from jax import lax

D_MODEL = 1024
D_FF = 512
EXPERTS = 32
TOP_K = 8
TOKENS_DEV = 2048
GROUP_DEVS = 32
EPS = 1e-5


def block_choice(block_key):
    mean_load = TOKENS_DEV * TOP_K // EXPERTS
    key_perm, key_delta, key_rows = jax.random.split(block_key, 3)
    expert_perm = jax.random.permutation(key_perm, EXPERTS)
    pair_delta = jax.random.randint(key_delta, (EXPERTS,), 0, mean_load)
    position = jnp.arange(EXPERTS)
    pair_index = jnp.maximum((position - 3) // 2, 0)
    pair_sign = jnp.where((position - 3) % 2 == 0, 1, -1)
    paired = (position >= 3) & (4 + 2 * pair_index < EXPERTS)
    load_delta = jnp.where(paired, pair_sign * pair_delta[pair_index], 0)
    load_delta = load_delta + jnp.where(position == 0, mean_load, 0) - jnp.where((position == 1) | (position == 2), mean_load // 2, 0)
    expert_loads = mean_load + load_delta
    run_ends = jnp.cumsum(expert_loads)
    flat_pos = jnp.arange(TOKENS_DEV * TOP_K)
    run_index = jnp.sum((flat_pos[:, None] >= run_ends[None, :]).astype(jnp.int32), axis=1)
    choice_grid = expert_perm[run_index].reshape(TOP_K, TOKENS_DEV).T
    row_perm = jax.random.permutation(key_rows, TOKENS_DEV)
    return choice_grid[row_perm].astype(jnp.int32)


def setup_inputs(seed: int = 0, part: int = 0) -> dict:
    weight_keys = jax.random.split(jax.random.key(seed), 6)
    part_key = jax.random.fold_in(jax.random.key(seed + 1), part)
    key_hidden, key_choice = jax.random.split(part_key)
    row_count = GROUP_DEVS * TOKENS_DEV
    hidden = jax.random.normal(key_hidden, (row_count, D_MODEL), jnp.float32).astype(jnp.bfloat16)
    choice = jax.vmap(block_choice)(jax.random.split(key_choice, GROUP_DEVS)).reshape(row_count, TOP_K)
    pre_scale = 1.0 + 0.5 * jax.random.normal(weight_keys[0], (D_MODEL,), jnp.float32)
    w_router = (jax.random.normal(weight_keys[1], (D_MODEL, EXPERTS), jnp.float32) * D_MODEL ** -0.5).astype(jnp.bfloat16)
    w_gelu = (jax.random.normal(weight_keys[2], (EXPERTS, D_MODEL, D_FF), jnp.float32) * D_MODEL ** -0.5).astype(jnp.bfloat16)
    w_linear = (jax.random.normal(weight_keys[3], (EXPERTS, D_MODEL, D_FF), jnp.float32) * D_MODEL ** -0.5).astype(jnp.bfloat16)
    w_down = (jax.random.normal(weight_keys[4], (EXPERTS, D_FF, D_MODEL), jnp.float32) * D_FF ** -0.5).astype(jnp.bfloat16)
    post_scale = 1.0 + 0.5 * jax.random.normal(weight_keys[5], (D_MODEL,), jnp.float32)
    return dict(hidden=hidden, choice=choice, pre_scale=pre_scale, w_router=w_router, w_gelu=w_gelu, w_linear=w_linear, w_down=w_down, post_scale=post_scale)


def rms_norm(values, gain_vec):
    return values * lax.rsqrt(jnp.mean(values * values, axis=-1, keepdims=True) + EPS) * gain_vec


def route_slots(block_ids, capacity):
    tok_rows, top_k = block_ids.shape
    flat_ids = block_ids.reshape(-1)
    sort_order = jnp.argsort(flat_ids, stable=True)
    counts = jnp.sum((flat_ids[:, None] == jnp.arange(EXPERTS)[None, :]).astype(jnp.int32), axis=0)
    starts = jnp.cumsum(counts) - counts
    slot_rank = jnp.arange(capacity)
    source = jnp.minimum(starts[:, None] + slot_rank[None, :], tok_rows * top_k - 1)
    slot_token = sort_order[source].reshape(-1) // top_k
    sorted_pos = jnp.argsort(sort_order, stable=True)
    slot_of = flat_ids * capacity + sorted_pos - starts[flat_ids]
    return slot_token, slot_of


def reference(hidden, choice, pre_scale, w_router, w_gelu, w_linear, w_down, post_scale):
    capacity = 2 * TOKENS_DEV * TOP_K // EXPERTS
    hidden_f = hidden.astype(jnp.float32)
    normed = rms_norm(hidden_f, pre_scale).astype(jnp.bfloat16)
    router_probs = jax.nn.softmax(jnp.dot(normed, w_router, preferred_element_type=jnp.float32), axis=-1)
    gate_vals = jnp.take_along_axis(router_probs, choice, axis=1)

    def one_expert(expert_args):
        expert_rows, gelu_w, linear_w, down_w = expert_args
        gelu_in = jnp.dot(expert_rows, gelu_w, preferred_element_type=jnp.float32)
        linear_in = jnp.dot(expert_rows, linear_w, preferred_element_type=jnp.float32)
        hidden_act = (jax.nn.gelu(gelu_in, approximate=True) * linear_in).astype(jnp.bfloat16)
        return jnp.dot(hidden_act, down_w, preferred_element_type=jnp.float32)

    def one_block(block_args):
        block_rows, block_ids, block_gates = block_args
        slot_token, slot_of = route_slots(block_ids, capacity)
        dispatched = jnp.take(block_rows, slot_token, axis=0).reshape(EXPERTS, capacity, D_MODEL)
        expert_out = lax.map(one_expert, (dispatched, w_gelu, w_linear, w_down)).reshape(EXPERTS * capacity, D_MODEL)
        picked = jnp.take(expert_out, slot_of, axis=0).reshape(TOKENS_DEV, TOP_K, D_MODEL)
        return jnp.sum(picked * block_gates[:, :, None], axis=1)

    mixed_out = lax.map(one_block, (normed.reshape(GROUP_DEVS, TOKENS_DEV, D_MODEL), choice.reshape(GROUP_DEVS, TOKENS_DEV, TOP_K), gate_vals.reshape(GROUP_DEVS, TOKENS_DEV, TOP_K))).reshape(GROUP_DEVS * TOKENS_DEV, D_MODEL)
    return (hidden_f + rms_norm(mixed_out, post_scale)).astype(jnp.bfloat16)
```

```python
import jax
import jax.numpy as jnp
from jax import lax
from jax.sharding import PartitionSpec as P

EPS = 1e-5
CHUNKS = 4


def rms_norm(values, gain_vec):
    return values * lax.rsqrt(jnp.mean(values * values, axis=-1, keepdims=True) + EPS) * gain_vec


def solution(mesh):
    def local_block(hidden, choice, pre_scale, w_router, w_gelu, w_linear, w_down, post_scale):
        num_experts = w_gelu.shape[0]
        per = num_experts // CHUNKS
        gelu_t = jnp.swapaxes(w_gelu, 1, 2)
        linear_t = jnp.swapaxes(w_linear, 1, 2)
        own = jnp.stack([gelu_t, linear_t, w_down], axis=1)
        hidden_f = hidden.astype(jnp.float32)
        normed = rms_norm(hidden_f, pre_scale).astype(jnp.bfloat16)
        probs = jax.nn.softmax(jnp.dot(normed, w_router, preferred_element_type=jnp.float32), axis=-1)
        chosen = jnp.any(choice[:, :, None] == jnp.arange(num_experts)[None, None, :], axis=1)
        gates = jnp.where(chosen, probs, -1.0)

        total = jnp.zeros(hidden.shape, jnp.float32)
        for c in range(CHUNKS):
            full = lax.all_gather(own[c * per:(c + 1) * per], 'wg', axis=2, tiled=True)

            def one(i, acc):
                w = lax.dynamic_index_in_dim(full, i, 0, keepdims=False)
                dims = (((1,), (1,)), ((), ()))
                u = lax.dot_general(normed, w[0], dims, preferred_element_type=jnp.float32)
                v = lax.dot_general(normed, w[1], dims, preferred_element_type=jnp.float32)
                act = (jax.nn.gelu(u, approximate=True) * v).astype(jnp.bfloat16)
                out = jnp.dot(act, w[2], preferred_element_type=jnp.float32)
                g = lax.dynamic_slice_in_dim(gates, c * per + i, 1, 1)
                return acc + jnp.where(g >= 0, g * out, 0.0)

            total = lax.fori_loop(0, per, one, total)
        return (hidden_f + rms_norm(total, post_scale)).astype(jnp.bfloat16)

    row_spec = P(('dp', 'wg'), None)
    weight_in = P(None, None, 'wg')
    return jax.shard_map(local_block, mesh=mesh, in_specs=(row_spec, row_spec, P(), P(), weight_in, weight_in, P(None, 'wg', None), P()), out_specs=row_spec, check_vma=False)
```

```python
import functools

import jax
import jax.numpy as jnp
from jax import lax
from jax.experimental import pallas as pl
from jax.experimental.pallas import tpu as pltpu
from jax.sharding import PartitionSpec as P

EPS = 1e-5
MESH = pl.DeviceIdType.MESH
PARTS = 4
LAG = dict(G=1, F=2, D=6, C=14, B=21)
BURST = 5
NT = (((1,), (1,)), ((), ()))


def moe_kernel(side, hidden, choice_t, pre_scale, router_t, gelu_t, linear_t, down, post_scale,
               out, gathered, rows_in, normed, total, gates, weights, own, staged,
               load_sem, own_sem, slot_sem, out_sem, send_sem, recv_a, recv_b, recv_c, recv_d, recv_f):
    experts, width, d_model = down.shape
    unit = 3 * width
    plane = side * side
    tokens = rows_in.shape[0]
    part = tokens // PARTS
    me = lax.axis_index('wg')
    core = me % 2
    x = (me // 2) % side
    y = me // (2 * side)
    partner = me + 1 - 2 * core
    ramp = -(-max(LAG.values()) // PARTS)

    def ring(e):
        odd = e % 2
        a = x + odd * (y - x)
        b = y + odd * (x - y)
        a_step = 2 + odd * (2 * side - 2)
        b_step = 2 * side - odd * (2 * side - 2)
        base = me - a * a_step - b * b_step
        def at(i, j):
            return base + ((i + side) % side) * a_step + ((j + side) % side) * b_step
        return a, b, at

    def spot(i, j):
        return core * plane + ((j + side) % side) * side + (i + side) % side

    def push(src, dst, e, recv, device):
        pltpu.make_async_remote_copy(
            src_ref=src, dst_ref=dst, send_sem=send_sem.at[e], recv_sem=recv.at[e],
            device_id={'wg': device}, device_id_type=MESH).start()

    def settle(sem, e, units):
        ref = gathered.at[e, pl.ds(0, units)]
        pltpu.make_async_copy(ref, ref, sem).wait()

    def row(e, j, first=0, count=side):
        return gathered.at[e, pl.ds(core * plane + ((j + side) % side) * side + first, count)]

    def stage_a(e):
        a, b, at = ring(e)
        dst = gathered.at[e, spot(a, b)]
        push(own.at[e], dst, e, recv_a, at(a + 1, b))
        push(own.at[e], dst, e, recv_a, at(a - 1, b))

    def stage_b(e):
        a, b, at = ring(e)
        settle(recv_a.at[e], e, 2)
        low = gathered.at[e, spot(a - 1, b), pl.ds(0, unit // 2)]
        push(low, low, e, recv_b, at(a + 1, b))
        high = gathered.at[e, spot(a + 1, b), pl.ds(unit // 2, unit // 2)]
        push(high, high, e, recv_b, at(a - 1, b))

    def stage_c(e):
        a, b, at = ring(e)
        settle(recv_b.at[e], e, 1)
        mine = row(e, b)
        push(mine, mine, e, recv_c, at(a, b + 1))
        push(mine, mine, e, recv_c, at(a, b - 1))
        push(mine, mine, e, recv_f, partner)

    def stage_d(e):
        a, b, at = ring(e)
        settle(recv_c.at[e], e, 2 * side)
        low = row(e, b - 1, 0, side // 2)
        push(low, low, e, recv_d, at(a, b + 1))
        high = row(e, b + 1, side // 2, side // 2)
        push(high, high, e, recv_d, at(a, b - 1))
        for j in (b - 1, b + 1):
            whole = row(e, j)
            push(whole, whole, e, recv_f, partner)

    def stage_f(e):
        a, b, at = ring(e)
        settle(recv_d.at[e], e, side)
        whole = row(e, b + 2)
        push(whole, whole, e, recv_f, partner)

    def fetch(e):
        slot = e % 2
        return pltpu.make_async_copy(gathered.at[e], weights.at[slot], slot_sem.at[slot])

    def stage_g(e):
        settle(recv_f.at[e], e, plane)
        fetch(e).start()

    stages = dict(G=stage_g, F=stage_f, D=stage_d, C=stage_c, B=stage_b)

    def serve(step, k):
        for name, lag in LAG.items():
            if (k + lag) % PARTS == 0:
                e = step + (k + lag) // PARTS

                @pl.when(jnp.logical_and(e >= 0, e < experts))
                def _():
                    stages[name](e)
        if k == 0:
            ahead = step + ramp + BURST

            @pl.when(ahead < experts)
            def _():
                stage_a(ahead)

    def router(first, count):
        rows = pl.ds(first, count)
        h = rows_in[rows, :].astype(jnp.float32)
        scale = lax.rsqrt(jnp.mean(h * h, axis=-1, keepdims=True) + EPS)
        n = (h * scale * pre_scale[...]).astype(jnp.bfloat16)
        normed[rows, :] = n
        logits = lax.dot_general(router_t[...], n, NT, preferred_element_type=jnp.float32)
        top = jnp.max(logits, axis=0, keepdims=True)
        p = jnp.exp(logits - top)
        p = p / jnp.sum(p, axis=0, keepdims=True)
        names = lax.broadcasted_iota(jnp.int32, p.shape, 0)
        picks = choice_t[:, rows]
        hit = names == picks[0:1, :]
        for j in range(1, picks.shape[0]):
            hit = jnp.logical_or(hit, names == picks[j:j + 1, :])
        g = jnp.where(hit, p, -1.0)
        g = jnp.concatenate([g, jnp.full((128 - experts, count), -1.0, jnp.float32)], axis=0)
        gates[rows, :] = g.T

    def compute(e, k, last):
        slot = e % 2
        rows = pl.ds(k * part, part)
        n = normed[rows, :]
        wide = 2 * plane * width
        u = lax.dot_general(n, weights[slot, :, 0:width, :].reshape(wide, d_model), NT, preferred_element_type=jnp.float32)
        v = lax.dot_general(n, weights[slot, :, width:2 * width, :].reshape(wide, d_model), NT, preferred_element_type=jnp.float32)
        act = (jax.nn.gelu(u, approximate=True) * v).astype(jnp.bfloat16)
        o = jnp.dot(act, weights[slot, :, 2 * width:, :].reshape(wide, d_model), preferred_element_type=jnp.float32)
        lanes = lax.broadcasted_iota(jnp.int32, (part, 128), 1)
        g = jnp.sum(jnp.where(lanes == e, gates[rows, :], 0.0), axis=1, keepdims=True)
        total[rows, :] += jnp.where(g >= 0.0, g * o, 0.0)

    barrier = pltpu.get_barrier_semaphore()
    _, _, at0 = ring(0)
    friends = [at0(x + 1, y), at0(x - 1, y), at0(x, y + 1), at0(x, y - 1), partner]
    for device in friends:
        pl.semaphore_signal(barrier, inc=1, device_id={'wg': device}, device_id_type=MESH)
    loads = [pltpu.make_async_copy(src, own.at[:, pl.ds(i * width, width), :], own_sem)
             for i, src in enumerate((gelu_t, linear_t, down))]
    for copy in loads:
        copy.start()
    load_rows = pltpu.make_async_copy(hidden, rows_in, load_sem)
    load_rows.start()
    for copy in loads:
        copy.wait()
    pl.semaphore_wait(barrier, len(friends))

    def early(e, carry):
        stage_a(e)
        return carry
    lax.fori_loop(0, BURST, early, 0)

    def keep(e, carry):
        a, b, _ = ring(e)
        pltpu.make_async_copy(own.at[e], gathered.at[e, spot(a, b)], own_sem).start()
        return carry
    lax.fori_loop(0, experts, keep, 0)
    pltpu.make_async_copy(own, own, own_sem).wait()
    load_rows.wait()

    blocks = 4
    span = tokens // blocks

    def warm(r, carry):
        for k in range(PARTS):
            serve(r - ramp, k)
            if k == 0:
                @pl.when(r < blocks)
                def _():
                    def some(i, c):
                        router(pl.multiple_of(r * span + i * 256, 256), 256)
                        return c
                    lax.fori_loop(0, span // 256, some, 0)
                    total[pl.ds(r * span, span), :] = jnp.zeros((span, d_model), jnp.float32)
        return carry
    lax.fori_loop(0, ramp, warm, 0)

    def step(e, carry):
        for k in range(PARTS):
            serve(e, k)
            if k == 0:
                fetch(e).wait()
            compute(e, k, False)
        return carry
    lax.fori_loop(0, experts, step, 0)

    piece = staged.shape[1]
    def finish(i, carry):
        rows = pl.ds(pl.multiple_of(i * piece, piece), piece)
        t = total[rows, :]
        scale = lax.rsqrt(jnp.mean(t * t, axis=-1, keepdims=True) + EPS)
        slot = i % 2

        @pl.when(i >= 2)
        def _():
            pltpu.make_async_copy(staged.at[slot], out.at[rows, :], out_sem.at[slot]).wait()
        staged[slot] = (rows_in[rows, :].astype(jnp.float32) + t * scale * post_scale[...]).astype(jnp.bfloat16)
        pltpu.make_async_copy(staged.at[slot], out.at[rows, :], out_sem.at[slot]).start()
        return carry
    lax.fori_loop(0, tokens // piece, finish, 0)
    for slot in range(2):
        pltpu.make_async_copy(staged.at[slot], out.at[pl.ds(0, piece), :], out_sem.at[slot]).wait()

    def drain(e, carry):
        settle(send_sem.at[e], e, 2 * plane - 1)
        return carry
    lax.fori_loop(0, experts, drain, 0)


def solution(mesh):
    group = mesh.shape['wg']
    side = int(round((group // 2) ** 0.5))

    def local_block(hidden, choice, pre_scale, w_router, w_gelu, w_linear, w_down, post_scale):
        tokens, d_model = hidden.shape
        experts, width, _ = w_down.shape
        unit = 3 * width
        vmem = pl.BlockSpec(memory_space=pltpu.VMEM)
        hbm = pl.BlockSpec(memory_space=pl.ANY)
        flops = 6 * tokens * experts * group * width * d_model
        result, _ = pl.pallas_call(
            functools.partial(moe_kernel, side),
            out_shape=(jax.ShapeDtypeStruct((tokens, d_model), jnp.bfloat16),
                       jax.ShapeDtypeStruct((experts, group, unit, d_model), jnp.bfloat16)),
            in_specs=[hbm, vmem, vmem, vmem, hbm, hbm, hbm, vmem],
            out_specs=(hbm, hbm),
            scratch_shapes=[
                pltpu.VMEM((tokens, d_model), jnp.bfloat16),
                pltpu.VMEM((tokens, d_model), jnp.bfloat16),
                pltpu.VMEM((tokens, d_model), jnp.float32),
                pltpu.VMEM((tokens, 128), jnp.float32),
                pltpu.VMEM((2, group, unit, d_model), jnp.bfloat16),
                pltpu.VMEM((experts, unit, d_model), jnp.bfloat16),
                pltpu.VMEM((2, 256, d_model), jnp.bfloat16),
                pltpu.SemaphoreType.DMA,
                pltpu.SemaphoreType.DMA,
                pltpu.SemaphoreType.DMA((2,)),
                pltpu.SemaphoreType.DMA((2,)),
                pltpu.SemaphoreType.DMA((experts,)),
                pltpu.SemaphoreType.DMA((experts,)),
                pltpu.SemaphoreType.DMA((experts,)),
                pltpu.SemaphoreType.DMA((experts,)),
                pltpu.SemaphoreType.DMA((experts,)),
                pltpu.SemaphoreType.DMA((experts,)),
            ],
            compiler_params=pltpu.CompilerParams(
                collective_id=0, has_side_effects=True, vmem_limit_bytes=62 * 1024 * 1024),
            cost_estimate=pl.CostEstimate(flops=flops, bytes_accessed=4 * experts * group * unit * d_model, transcendentals=0),
            name='moe',
        )(hidden, choice.T, pre_scale.reshape(1, -1), w_router.T, jnp.swapaxes(w_gelu, 1, 2),
          jnp.swapaxes(w_linear, 1, 2), w_down, post_scale.reshape(1, -1))
        return result

    row_spec = P(('dp', 'wg'), None)
    weight_in = P(None, None, 'wg')
    return jax.shard_map(local_block, mesh=mesh, in_specs=(row_spec, row_spec, P(), P(), weight_in, weight_in, P(None, 'wg', None), P()), out_specs=row_spec, check_vma=False)
```

```python
import functools

import jax
import jax.numpy as jnp
from jax import lax
from jax.experimental import pallas as pl
from jax.experimental.pallas import tpu as pltpu
from jax.sharding import PartitionSpec as P

EPS = 1e-5
GELU_A = 0.7978845608028654
GELU_B = GELU_A * 0.044715
MESH = pl.DeviceIdType.MESH
HALVES = 2
BLOCKS = (1024, 1024)
LAG = dict(G=1, F=2, D=4, C=7, B=9)
BURST = 8
NT = (((1,), (1,)), ((), ()))


def moe_kernel(side, hidden, choice_t, pre_scale, router_t, gelu_t, linear_t, down, post_scale,
               out, gathered, rows_in, normed, total, gates, weights, own, staged,
               load_sem, own_sem, slot_sem, out_sem, send_sem, recv_a, recv_b, recv_c, recv_d, recv_f):
    steps, unit, d_model = down.shape
    experts = steps // HALVES
    plane = side * side
    wide = 2 * plane * unit
    tokens = rows_in.shape[0]
    me = lax.axis_index('wg')
    core = me % 2
    x = (me // 2) % side
    y = me // (2 * side)

    def device(i, j, c):
        return (((j + side) % side) * side + (i + side) % side) * 2 + c
    partner = device(x, y, 1 - core)
    along_x = (device(x + 1, y, core), device(x - 1, y, core))
    along_y = (device(x, y + 1, core), device(x, y - 1, core))
    rings = ((x, y, along_x, along_y), (y, x, along_y, along_x))
    ramp = -(-max(LAG.values()) // HALVES) * HALVES

    def units(s, j, i=0, count=side):
        first = core * plane + ((j + side) % side) * side + (i + side) % side
        return gathered.at[s, :, pl.ds(pl.multiple_of(first * unit, unit), count * unit)]

    def push(src, dst, s, recv, target):
        pltpu.make_async_remote_copy(
            src_ref=src, dst_ref=dst, send_sem=send_sem.at[s], recv_sem=recv.at[s],
            device_id={'wg': target}, device_id_type=MESH).start()

    def settle(sem, s, count):
        ref = gathered.at[s, :, pl.ds(0, count * unit)]
        pltpu.make_async_copy(ref, ref, sem).wait()

    def stage_a(s, parity):
        a, b, first, _ = rings[parity]
        for target in first:
            push(own.at[s], units(s, b, a, 1), s, recv_a, target)

    def stage_b(s, parity):
        a, b, first, _ = rings[parity]
        settle(recv_a.at[s], s, 2)
        half = d_model // 2
        for i, target in ((0, first[0]), (1, first[1])):
            piece = units(s, b, a - 1 + 2 * i, 1).at[:, :, pl.ds(i * half, half)]
            push(piece, piece, s, recv_b, target)

    def stage_c(s, parity):
        a, b, _, second = rings[parity]
        settle(recv_b.at[s], s, 1)
        mine = units(s, b)
        for target in second:
            push(mine, mine, s, recv_c, target)
        push(mine, mine, s, recv_f, partner)

    def stage_d(s, parity):
        a, b, _, second = rings[parity]
        settle(recv_c.at[s], s, 2 * side)
        for i, target in ((0, second[0]), (1, second[1])):
            piece = units(s, b - 1 + 2 * i, i * (side // 2), side // 2)
            push(piece, piece, s, recv_d, target)
        for j in (b - 1, b + 1):
            piece = units(s, j)
            push(piece, piece, s, recv_f, partner)

    def stage_f(s, parity):
        a, b, _, second = rings[parity]
        settle(recv_d.at[s], s, side)
        piece = units(s, b + 2)
        push(piece, piece, s, recv_f, partner)

    def fetch(s, slot):
        return pltpu.make_async_copy(gathered.at[s], weights.at[slot], slot_sem.at[slot])

    def stage_g(s, parity):
        settle(recv_f.at[s], s, plane)
        fetch(s, parity).start()

    stages = dict(G=stage_g, F=stage_f, D=stage_d, C=stage_c, B=stage_b)

    def serve(pair, half):
        for name, lag in LAG.items():
            s = pair * HALVES + half + lag

            @pl.when(jnp.logical_and(s >= 0, s < steps))
            def _():
                stages[name](s, (half + lag) % 2)
        s = pair * HALVES + half + ramp + BURST

        @pl.when(s < steps)
        def _():
            stage_a(s, half)

    def router(first, count):
        rows = pl.ds(first, count)
        h = rows_in[rows, :].astype(jnp.float32)
        scale = lax.rsqrt(jnp.mean(h * h, axis=-1, keepdims=True) + EPS)
        n = (h * scale * pre_scale[...]).astype(jnp.bfloat16)
        normed[rows, :] = n
        logits = lax.dot_general(router_t[...], n, NT, preferred_element_type=jnp.float32)
        top = jnp.max(logits, axis=0, keepdims=True)
        p = jnp.exp(logits - top)
        p = p / jnp.sum(p, axis=0, keepdims=True)
        names = lax.broadcasted_iota(jnp.int32, p.shape, 0)
        picks = choice_t[:, rows]
        hit = names == picks[0:1, :]
        for j in range(1, picks.shape[0]):
            hit = jnp.logical_or(hit, names == picks[j:j + 1, :])
        g = jnp.where(hit, p, -1.0)
        g = jnp.concatenate([g, jnp.full((128 - experts, count), -1.0, jnp.float32)], axis=0)
        gates[rows, :] = g.T

    sizes = [tokens * size // sum(BLOCKS) for size in BLOCKS]
    starts = [sum(sizes[:i]) for i in range(len(sizes))]

    def compute(e, half):
        up = weights[half, 0:2].reshape(2 * wide, d_model)
        held = []

        def rise(i):
            rows = pl.ds(starts[i], sizes[i])
            uv = lax.dot_general(normed[rows, :], up, NT, preferred_element_type=jnp.float32)
            u, v = uv[:, :wide], uv[:, wide:]
            lanes = lax.broadcasted_iota(jnp.int32, (sizes[i], 128), 1)
            g = jnp.sum(jnp.where(lanes == e, gates[rows, :], 0.0), axis=1, keepdims=True)
            bent = jnp.tanh(u * (GELU_A + GELU_B * (u * u)))
            flat = 0.5 * u
            act = jnp.where(g >= 0.0, (flat + flat * bent) * v, 0.0).astype(jnp.bfloat16)
            held.append((act, jnp.maximum(g, 0.0)))

        def fall(i):
            rows = pl.ds(starts[i], sizes[i])
            act, g = held[i]
            total[rows, :] += g * jnp.dot(act, weights[half, 2], preferred_element_type=jnp.float32)

        rise(0)
        for i in range(1, len(sizes)):
            rise(i)
            fall(i - 1)
        fall(len(sizes) - 1)

    barrier = pltpu.get_barrier_semaphore()
    friends = along_x + along_y + (partner,)
    for target in friends:
        pl.semaphore_signal(barrier, inc=1, device_id={'wg': target}, device_id_type=MESH)
    loads = [pltpu.make_async_copy(src, own.at[:, i], own_sem)
             for i, src in enumerate((gelu_t, linear_t, down))]
    for copy in loads:
        copy.start()
    load_rows = pltpu.make_async_copy(hidden, rows_in, load_sem)
    load_rows.start()
    for copy in loads:
        copy.wait()
    pl.semaphore_wait(barrier, len(friends))

    def early(i, carry):
        for half in range(HALVES):
            stage_a(i * HALVES + half, half)
        return carry
    lax.fori_loop(0, BURST // HALVES, early, 0)

    def keep(i, carry):
        for half in range(HALVES):
            s = i * HALVES + half
            a, b, _, _ = rings[half]
            pltpu.make_async_copy(own.at[s], units(s, b, a, 1), own_sem).start()
        return carry
    lax.fori_loop(0, experts, keep, 0)
    pltpu.make_async_copy(own, own, own_sem).wait()
    load_rows.wait()

    blocks = 4
    span = tokens // blocks

    def warm(r, carry):
        for half in range(HALVES):
            serve(r - ramp // HALVES, half)
            if half == 0:
                @pl.when(r < blocks)
                def _():
                    def some(i, c):
                        router(pl.multiple_of(r * span + i * 256, 256), 256)
                        return c
                    lax.fori_loop(0, span // 256, some, 0)
                    total[pl.ds(r * span, span), :] = jnp.zeros((span, d_model), jnp.float32)
        return carry
    lax.fori_loop(0, ramp // HALVES, warm, 0)

    def step(e, carry):
        for half in range(HALVES):
            serve(e, half)
            fetch(e * HALVES + half, half).wait()
            compute(e, half)
        return carry
    lax.fori_loop(0, experts, step, 0)

    piece = staged.shape[1]

    def finish(i, carry):
        rows = pl.ds(pl.multiple_of(i * piece, piece), piece)
        t = total[rows, :]
        scale = lax.rsqrt(jnp.mean(t * t, axis=-1, keepdims=True) + EPS)
        slot = i % 2

        @pl.when(i >= 2)
        def _():
            pltpu.make_async_copy(staged.at[slot], out.at[rows, :], out_sem.at[slot]).wait()
        staged[slot] = (rows_in[rows, :].astype(jnp.float32) + t * scale * post_scale[...]).astype(jnp.bfloat16)
        pltpu.make_async_copy(staged.at[slot], out.at[rows, :], out_sem.at[slot]).start()
        return carry
    lax.fori_loop(0, tokens // piece, finish, 0)
    for slot in range(2):
        pltpu.make_async_copy(staged.at[slot], out.at[pl.ds(0, piece), :], out_sem.at[slot]).wait()

    def drain(s, carry):
        settle(send_sem.at[s], s, 2 * plane - 1)
        return carry
    lax.fori_loop(0, steps, drain, 0)


def solution(mesh):
    group = mesh.shape['wg']
    side = int(round((group // 2) ** 0.5))

    def local_block(hidden, choice, pre_scale, w_router, w_gelu, w_linear, w_down, post_scale):
        tokens, d_model = hidden.shape
        experts, width, _ = w_down.shape
        steps, unit = experts * HALVES, width // HALVES
        wide = group * unit
        vmem = pl.BlockSpec(memory_space=pltpu.VMEM)
        hbm = pl.BlockSpec(memory_space=pl.ANY)
        flops = 6 * tokens * experts * group * width * d_model
        result, _ = pl.pallas_call(
            functools.partial(moe_kernel, side),
            out_shape=(jax.ShapeDtypeStruct((tokens, d_model), jnp.bfloat16),
                       jax.ShapeDtypeStruct((steps, 3, wide, d_model), jnp.bfloat16)),
            in_specs=[hbm, vmem, vmem, vmem, hbm, hbm, hbm, vmem],
            out_specs=(hbm, hbm),
            scratch_shapes=[
                pltpu.VMEM((tokens, d_model), jnp.bfloat16),
                pltpu.VMEM((tokens, d_model), jnp.bfloat16),
                pltpu.VMEM((tokens, d_model), jnp.float32),
                pltpu.VMEM((tokens, 128), jnp.float32),
                pltpu.VMEM((HALVES, 3, wide, d_model), jnp.bfloat16),
                pltpu.VMEM((steps, 3, unit, d_model), jnp.bfloat16),
                pltpu.VMEM((2, 256, d_model), jnp.bfloat16),
                pltpu.SemaphoreType.DMA,
                pltpu.SemaphoreType.DMA,
                pltpu.SemaphoreType.DMA((HALVES,)),
                pltpu.SemaphoreType.DMA((2,)),
            ] + [pltpu.SemaphoreType.DMA((steps,))] * 6,
            compiler_params=pltpu.CompilerParams(
                collective_id=0, has_side_effects=True, vmem_limit_bytes=62 * 1024 * 1024),
            cost_estimate=pl.CostEstimate(flops=flops, bytes_accessed=4 * steps * 3 * wide * d_model, transcendentals=0),
            name='moe',
        )(hidden, choice.T, pre_scale.reshape(1, -1), w_router.T,
          jnp.swapaxes(w_gelu, 1, 2).reshape(steps, unit, d_model),
          jnp.swapaxes(w_linear, 1, 2).reshape(steps, unit, d_model),
          w_down.reshape(steps, unit, d_model), post_scale.reshape(1, -1))
        return result

    row_spec = P(('dp', 'wg'), None)
    weight_in = P(None, None, 'wg')
    return jax.shard_map(local_block, mesh=mesh, in_specs=(row_spec, row_spec, P(), P(), weight_in, weight_in, P(None, 'wg', None), P()), out_specs=row_spec, check_vma=False)
```
